256 devices in a mesh: ep: 8 (over y, core), fsdp: 32 (over z, x).
Axes of the slice: x: 4, y: 4, z: 8, core: 2. Of those that a mesh axis runs over, the one named last changes fastest.
Arguments:
- w_down: float32 [16, 6400, 4096], P('ep', None, 'fsdp'), may hold values from -0.15625 to 0.15625
- router_weight: float32 [4096, 16], P('fsdp', 'ep'), may hold values from -0.09375 to 0.09375
- router_gain: float32 [4096], P('fsdp'), may hold values from 0.25 to 1.75
Outputs:
- serve_down: bfloat16 [16, 6400, 4096], P('ep', 'fsdp')
- scale_down: float32 [16, 6400], P('ep', 'fsdp')
- serve_router: bfloat16 [4096, 16], replicated
The draws below stay inside these ranges and needn't reach their ends.
All inputs are finite; a program needn't handle non-finite values.
Results may differ from the reference program's by a relative error of at most 0.001.
Values may be sent and summed in bfloat16 or wider, within the bound.
A program may use at most 64 MiB of HBM per device.

```python
import jax
import jax.numpy as jnp
from jax import lax

EXPERTS = 16
D_MODEL = 4096
D_EXPERT = 6400


def strengthened(entries, key, source, target, parts, factor):
    def block_of(axis_at):
        return (jnp.arange(entries.shape[axis_at]) // (entries.shape[axis_at] // parts)).reshape((-1,) + (1,) * (entries.ndim - 1 - axis_at))

    near = jax.random.permutation(key, parts)[block_of(target)]
    second = (block_of(target) + parts // 2) % parts
    return jnp.where((block_of(source) == near) | (block_of(source) == second), factor * entries, entries)


def shard_levels(stream_key, extent, cuts, low, high):
    gain = 1.0
    for position, parts in cuts:
        heights = jax.random.uniform(jax.random.fold_in(jax.random.fold_in(stream_key, 6), position), (parts,), jnp.float32, low / len(cuts), high / len(cuts))
        gain = gain * jnp.repeat(jnp.exp(heights), extent[position] // parts).reshape((-1,) + (1,) * (len(extent) - 1 - position))
    return gain


def scatter_about(rng, extent, width, limit, pieces=(), held_as=jnp.bfloat16):
    entries = width * jax.random.normal(rng, extent, jnp.float32)
    if pieces:
        entries = entries * shard_levels(rng, extent, pieces, -0.22, 0.18)
    return jnp.clip(entries, -limit, limit).astype(held_as)


def heavy_noise(own_key, dims, deviation, limit, shards, heavy, held_as=jnp.bfloat16):
    array = deviation * jax.random.normal(own_key, dims, jnp.float32)
    if shards:
        array = array * shard_levels(own_key, dims, shards, -0.22, 0.18)
    return jnp.clip(strengthened(array, jax.random.fold_in(own_key, 3), *heavy), -limit, limit).astype(held_as)


def setup_inputs(seed: int = 0) -> dict:
    arg_keys = jax.random.split(jax.random.key(seed), 4)
    return {
        "w_down": heavy_noise(arg_keys[0], (EXPERTS, D_EXPERT, D_MODEL), D_EXPERT ** -0.5, 0.15625, ((0, 8), (2, 32)), (2, 1, 32, 2.75), jnp.float32),
        "router_weight": scatter_about(arg_keys[1], (D_MODEL, EXPERTS), D_MODEL ** -0.5, 0.09375, ((0, 32), (1, 8)), jnp.float32),
        "router_gain": jnp.clip(1.0 + 0.15 * jax.random.normal(arg_keys[2], (D_MODEL,), jnp.float32), 0.25, 1.75),
    }


def reference(w_down, router_weight, router_gain):
    scale_down = jnp.sqrt(lax.optimization_barrier(jnp.sum(w_down * w_down, axis=2)))
    serve_down = (w_down / jnp.expand_dims(scale_down, 2)).astype(jnp.bfloat16)
    serve_router = (router_weight * router_gain[:, None]).astype(jnp.bfloat16)
    return (serve_down, scale_down, serve_router)
```

```python
import functools

import jax
import jax.numpy as jnp
from jax import lax
from jax.experimental import pallas as pl
from jax.experimental.pallas import tpu as pltpu
from jax.sharding import PartitionSpec as P

MESH = pl.DeviceIdType.MESH
F32, BF16 = jnp.float32, jnp.bfloat16
CHUNKS = 4


def peer(k, z, x):
    j, dx = k // 4, lax.rem(k, 4)
    odd = lax.rem(j, 2)
    dz = odd * ((j + 1) // 2) + (1 - odd) * (8 - j // 2)
    return lax.rem(z + dz, 8) * 4 + lax.rem(x + dx, 4)


def row_sums(block):
    square = block * block
    high = square.astype(BF16)
    rest = square - high.astype(F32)
    middle = rest.astype(BF16)
    low = (rest - middle.astype(F32)).astype(BF16)
    ones = jnp.ones((8, 128), BF16)
    dot = lambda part: lax.dot_general(
        ones, part, (((1,), (1,)), ((), ())), preferred_element_type=F32
    )
    return (dot(high) + dot(middle) + dot(low))[:1]


def kernel(
    w_ref, router_ref, gain_ref, down_ref, scale_ref, serve_router_ref,
    w, part, landed, total, scales, send, rows, columns,
    load_sem, part_send, part_recv, scale_send, scale_recv,
    down_send, down_recv, router_send, router_recv,
):
    n, width = 32, 200
    ep, me = lax.axis_index("ep"), lax.axis_index("fsdp")
    z, x = me // 4, lax.rem(me, 4)

    span = 6400 // CHUNKS
    loads = [
        pltpu.make_async_copy(
            w_ref.at[:, pl.ds(c * span, span), :], w.at[:, pl.ds(c * span, span), :], load_sem.at[c]
        )
        for c in range(CHUNKS)
    ]
    for load in loads:
        load.start()

    barrier = pltpu.get_barrier_semaphore()

    @pl.loop(1, n)
    def _(k):
        pl.semaphore_signal(barrier, inc=1, device_id={"fsdp": peer(k, z, x)}, device_id_type=MESH)

    @pl.loop(1, 8)
    def _(k):
        pl.semaphore_signal(barrier, inc=1, device_id={"ep": lax.rem(ep + k, 8)}, device_id_type=MESH)

    router = router_ref[...] * gain_ref[...]

    for c in range(CHUNKS):
        loads[c].wait()

        @pl.loop(c * (n // CHUNKS), (c + 1) * (n // CHUNKS))
        def _(t):
            block = w[:, pl.ds(pl.multiple_of(t * width, 8), width), :].reshape(2 * width, 128)
            part[t, :, 0:400] = row_sums(block)
            part[t, :, 512:640] = router[0:1]
            part[t, :, 640:768] = router[1:2]

    pl.semaphore_wait(barrier, 38)

    @pl.loop(1, n)
    def _(k):
        t = peer(k, z, x)
        pltpu.make_async_remote_copy(
            src_ref=part.at[t], dst_ref=landed.at[me], send_sem=part_send, recv_sem=part_recv,
            device_id={"fsdp": t}, device_id_type=MESH,
        ).start()

    landed[me] = part[me]
    pltpu.make_async_copy(landed.at[pl.ds(0, n - 1)], landed.at[pl.ds(0, n - 1)], part_recv).wait()
    scale = jnp.sqrt(jnp.sum(landed[:, :, 0:512], axis=0))
    total[...] = scale
    scales[me] = scale
    scale_ref[0:1] = scale[:, 0:width]
    scale_ref[1:2] = scale[:, width : 2 * width]

    @pl.loop(0, n)
    def _(s):
        lanes = pl.ds(pl.multiple_of(s * 128, 128), 128)
        rows[0:1, lanes] = landed[s, :, 512:640]
        rows[1:2, lanes] = landed[s, :, 640:768]

    @pl.loop(1, n)
    def _(k):
        t = peer(k, z, x)
        pltpu.make_async_remote_copy(
            src_ref=total, dst_ref=scales.at[me], send_sem=scale_send, recv_sem=scale_recv,
            device_id={"fsdp": t}, device_id_type=MESH,
        ).start()

    @pl.loop(1, 8)
    def _(k):
        pltpu.make_async_remote_copy(
            src_ref=rows, dst_ref=columns.at[ep], send_sem=router_send, recv_sem=router_recv,
            device_id={"ep": lax.rem(ep + k, 8)}, device_id_type=MESH,
        ).start()

    columns[ep] = rows[...]
    pltpu.make_async_copy(scales.at[pl.ds(0, n - 1)], scales.at[pl.ds(0, n - 1)], scale_recv).wait()

    def scaled(t):
        inverse = 1.0 / scales[t][:, 0:400]
        block = w[:, pl.ds(pl.multiple_of(t * width, 8), width), :].reshape(2 * width, 128)
        return (block * jnp.broadcast_to(inverse, (128, 400)).T).astype(BF16)

    lanes = pl.ds(pl.multiple_of(me * 128, 128), 128)

    def go(k):
        t = peer(k, z, x)
        pltpu.make_async_remote_copy(
            src_ref=send.at[t], dst_ref=down_ref.at[:, :, lanes], send_sem=down_send, recv_sem=down_recv,
            device_id={"fsdp": t}, device_id_type=MESH,
        ).start()

    @pl.loop(1, n)
    def _(k):
        t = peer(k, z, x)
        value = scaled(t)
        send[t, 0] = value[0:width]
        send[t, 1] = value[width:]

        @pl.when(k > 1)
        def _():
            go(k - 1)

    own = scaled(me)
    down_ref[0, :, lanes] = own[0:width]
    down_ref[1, :, lanes] = own[width:]
    go(n - 1)

    pltpu.make_async_copy(columns.at[pl.ds(0, 7)], columns.at[pl.ds(0, 7)], router_recv).wait()
    for e in range(8):
        serve_router_ref[2 * e : 2 * e + 2, :] = columns[e].astype(BF16)

    pltpu.make_async_copy(part.at[pl.ds(0, n - 1)], part.at[pl.ds(0, n - 1)], part_send).wait()
    pltpu.make_async_copy(scales.at[pl.ds(0, n - 1)], scales.at[pl.ds(0, n - 1)], scale_send).wait()
    pltpu.make_async_copy(columns.at[pl.ds(0, 7)], columns.at[pl.ds(0, 7)], router_send).wait()
    pltpu.make_async_copy(send.at[pl.ds(0, n - 1)], send.at[pl.ds(0, n - 1)], down_send).wait()
    pltpu.make_async_copy(send.at[pl.ds(0, n - 1)], send.at[pl.ds(0, n - 1)], down_recv).wait()


def body(w_down, router_weight, router_gain):
    vmem, hbm = pl.BlockSpec(memory_space=pltpu.VMEM), pl.BlockSpec(memory_space=pltpu.HBM)
    dma = pltpu.SemaphoreType.DMA
    down, scale, router = pl.pallas_call(
        kernel,
        out_shape=(
            jax.ShapeDtypeStruct((2, 200, 4096), BF16),
            jax.ShapeDtypeStruct((2, 200), F32),
            jax.ShapeDtypeStruct((16, 4096), BF16),
        ),
        in_specs=[hbm, vmem, vmem],
        out_specs=(vmem, vmem, vmem),
        scratch_shapes=[
            pltpu.VMEM((2, 6400, 128), F32),
            pltpu.VMEM((32, 1, 768), F32),
            pltpu.VMEM((32, 1, 768), F32),
            pltpu.VMEM((1, 512), F32),
            pltpu.VMEM((32, 1, 512), F32),
            pltpu.VMEM((32, 2, 200, 128), BF16),
            pltpu.VMEM((2, 4096), F32),
            pltpu.VMEM((8, 2, 4096), F32),
            dma((CHUNKS,)), dma, dma, dma, dma, dma, dma, dma, dma,
        ],
        compiler_params=pltpu.CompilerParams(
            collective_id=0, has_side_effects=True, vmem_limit_bytes=62_000_000
        ),
        name="serve",
    )(w_down, router_weight.T, router_gain[None])
    return down, scale, router.T


def solution(mesh):
    return jax.shard_map(
        body,
        mesh=mesh,
        in_specs=(P("ep", None, "fsdp"), P("fsdp", "ep"), P("fsdp")),
        out_specs=(P("ep", "fsdp", None), P("ep", "fsdp"), P()),
        check_vma=False,
    )
```

```python
import jax
import jax.numpy as jnp
from jax import lax
from jax.experimental import pallas as pl
from jax.experimental.pallas import tpu as pltpu
from jax.sharding import PartitionSpec as P

MESH = pl.DeviceIdType.MESH
F32, BF16 = jnp.float32, jnp.bfloat16
Z, X, EP = 8, 4, 8
PARTNERS = Z * X
ROWS = 200
CHUNKS = 4
VMEM_LIMIT = 40_000_000

NEAR = sorted(
    ((dz, dx) for dz in range(Z) for dx in range(X) if dz or dx),
    key=lambda o: (min(o[0], Z - o[0]) + min(o[1], X - o[1]), o),
)


def stretches(z, x):
    def at(dz, dx):
        return lax.rem(z + dz, Z) * X + lax.rem(x + dx, X)

    def close(i):
        return at(1 + 6 * lax.rem(i, 2), i // 2)

    def wide(i):
        j = lax.rem(i, 6)
        odd = lax.rem(j, 2)
        return at((1 - odd) * (4 + j // 2) + odd * (4 - (j + 1) // 2 - j // 5), 3 - i // 6)

    return (8, close), (23, wide)


def row_sums(block):
    square = block * block
    total = jnp.broadcast_to(jnp.sum(square, axis=1, keepdims=True), square.shape)
    rows = lax.broadcasted_iota(jnp.int32, (128, 128), 0)
    own = rows == lax.broadcasted_iota(jnp.int32, (128, 128), 1)
    return jnp.concatenate(
        [
            jnp.sum(
                jnp.where(own[: min(128, 2 * ROWS - r)], total[r : r + 128], 0.0),
                axis=0,
                keepdims=True,
            )
            for r in range(0, 2 * ROWS, 128)
        ],
        axis=1,
    )


def serve(
    w_ref, weight_ref, gain_ref, down_ref, scale_ref, router_ref,
    w, weight, gain, part, landed, total, scales, send, rows, columns,
    load_sem, part_send, part_recv, scale_send, scale_recv,
    down_send, down_recv, router_send, router_recv,
):
    ep, me = lax.axis_index("ep"), lax.axis_index("fsdp")
    z, x = me // X, lax.rem(me, X)

    span = PARTNERS * ROWS // CHUNKS
    loads = []
    for c in range(CHUNKS):
        piece = pl.ds(c * span, span)
        loads.append((w_ref.at[:, piece, :], w.at[:, piece, :]))
    loads += [(weight_ref, weight), (gain_ref, gain)]
    loads = [pltpu.make_async_copy(*pair, load_sem.at[i]) for i, pair in enumerate(loads)]
    for load in loads:
        load.start()

    barrier = pltpu.get_barrier_semaphore()
    zs = [lax.rem(z + d, Z) * X for d in range(Z)]
    xs = [lax.rem(x + d, X) for d in range(X)]
    partners = [zs[dz] + xs[dx] for dz, dx in NEAR]
    peers = [lax.rem(ep + d, EP) for d in range(1, EP)]
    for t in reversed(partners):
        pl.semaphore_signal(barrier, inc=1, device_id={"fsdp": t}, device_id_type=MESH)
    for e in peers:
        pl.semaphore_signal(barrier, inc=1, device_id={"ep": e}, device_id_type=MESH)

    loads[CHUNKS].wait()
    loads[CHUNKS + 1].wait()
    router = weight[...] * gain[...]

    def rows_of(t):
        block = w[:, pl.ds(pl.multiple_of(t * ROWS, 8), ROWS), :]
        return block.reshape(2 * ROWS, 128)

    for c in range(CHUNKS):
        loads[c].wait()
        each = PARTNERS // CHUNKS

        @pl.loop(c * each, (c + 1) * each, unroll=each)
        def _(t):
            part[t, :, 0:512] = row_sums(rows_of(t))
            part[t, :, 512:640] = router[0:1]
            part[t, :, 640:768] = router[1:2]

    pl.semaphore_wait(barrier, len(partners) + len(peers))
    for t in reversed(partners):
        pltpu.make_async_remote_copy(
            src_ref=part.at[t], dst_ref=landed.at[me], send_sem=part_send, recv_sem=part_recv,
            device_id={"fsdp": t}, device_id_type=MESH,
        ).start()

    landed[me] = part[me]
    others = pl.ds(0, PARTNERS - 1)
    pltpu.make_async_copy(landed.at[others], landed.at[others], part_recv).wait()
    scale = jnp.sqrt(jnp.sum(landed[:, :, 0:512], axis=0))
    total[...] = scale
    scales[me] = scale
    for e in range(2):
        scale_ref[e : e + 1] = scale[:, e * ROWS : (e + 1) * ROWS]
    for t in partners:
        pltpu.make_async_remote_copy(
            src_ref=total, dst_ref=scales.at[me], send_sem=scale_send, recv_sem=scale_recv.at[me],
            device_id={"fsdp": t}, device_id_type=MESH,
        ).start()

    @pl.loop(0, PARTNERS)
    def _(s):
        lanes = pl.ds(pl.multiple_of(s * 128, 128), 128)
        rows[0:1, lanes] = landed[s, :, 512:640]
        rows[1:2, lanes] = landed[s, :, 640:768]

    columns[ep] = rows[...]
    for e in peers:
        pltpu.make_async_remote_copy(
            src_ref=rows, dst_ref=columns.at[ep], send_sem=router_send, recv_sem=router_recv,
            device_id={"ep": e}, device_id_type=MESH,
        ).start()

    lanes = pl.ds(pl.multiple_of(me * 128, 128), 128)

    def scaled(t):
        inverse = 1.0 / scales[t, :, 0 : 2 * ROWS]
        return (rows_of(t) * jnp.broadcast_to(inverse, (128, 2 * ROWS)).T).astype(BF16)

    def make(t):
        pltpu.make_async_copy(scales.at[t], scales.at[t], scale_recv.at[t]).wait()
        value = scaled(t)
        send[t, 0] = value[:ROWS]
        send[t, 1] = value[ROWS:]

    def go(t):
        pltpu.make_async_remote_copy(
            src_ref=send.at[t], dst_ref=down_ref.at[:, :, lanes], send_sem=down_send, recv_sem=down_recv,
            device_id={"fsdp": t}, device_id_type=MESH,
        ).start()

    for count, partner in stretches(z, x):
        make(partner(0))

        @pl.loop(1, count)
        def _(i):
            make(partner(i))
            go(partner(i - 1))

        go(partner(count - 1))

    own = scaled(me)
    down_ref[0, :, lanes] = own[:ROWS]
    down_ref[1, :, lanes] = own[ROWS:]

    pltpu.make_async_copy(columns.at[pl.ds(0, EP - 1)], columns.at[pl.ds(0, EP - 1)], router_recv).wait()
    for e in range(EP):
        router_ref[2 * e : 2 * e + 2, :] = columns[e].astype(BF16)

    pltpu.make_async_copy(part.at[others], part.at[others], part_send).wait()
    pltpu.make_async_copy(scales.at[others], scales.at[others], scale_send).wait()
    pltpu.make_async_copy(columns.at[pl.ds(0, EP - 1)], columns.at[pl.ds(0, EP - 1)], router_send).wait()
    pltpu.make_async_copy(send.at[others], send.at[others], down_send).wait()
    pltpu.make_async_copy(send.at[others], send.at[others], down_recv).wait()


def put_out(down_ref, scale_ref, router_ref, down_out, scale_out, router_out, sem):
    pairs = [(scale_ref, scale_out), (router_ref, router_out)]
    for e in range(2):
        for r in range(0, ROWS, 40):
            piece = pl.ds(r, 40)
            pairs.append((down_ref.at[e, piece], down_out.at[e, piece]))
    copies = [pltpu.make_async_copy(*pair, sem.at[i]) for i, pair in enumerate(pairs)]
    for copy in copies:
        copy.start()
    for copy in copies:
        copy.wait()


def body(w_down, router_weight, router_gain):
    vmem, hbm = pl.BlockSpec(memory_space=pltpu.VMEM), pl.BlockSpec(memory_space=pltpu.HBM)
    dma = pltpu.SemaphoreType.DMA
    outs = (
        jax.ShapeDtypeStruct((2, ROWS, PARTNERS * 128), BF16),
        jax.ShapeDtypeStruct((2, ROWS), F32),
        jax.ShapeDtypeStruct((2 * EP, PARTNERS * 128), BF16),
    )
    operands = (w_down, router_weight.T, router_gain[None])
    served = pl.pallas_call(
        serve,
        out_shape=outs,
        in_specs=[hbm] * 3,
        out_specs=(vmem,) * 3,
        scratch_shapes=[
            pltpu.VMEM((2, PARTNERS * ROWS, 128), F32),
            pltpu.VMEM((2, 128), F32),
            pltpu.VMEM((1, 128), F32),
            pltpu.VMEM((PARTNERS, 1, 768), F32),
            pltpu.VMEM((PARTNERS, 1, 768), F32),
            pltpu.VMEM((1, 512), F32),
            pltpu.VMEM((PARTNERS, 1, 512), F32),
            pltpu.VMEM((PARTNERS, 2, ROWS, 128), BF16),
            pltpu.VMEM((2, PARTNERS * 128), F32),
            pltpu.VMEM((EP, 2, PARTNERS * 128), F32),
            dma((CHUNKS + 2,)), dma, dma, dma, dma((PARTNERS,)), dma, dma, dma, dma,
        ],
        compiler_params=pltpu.CompilerParams(
            collective_id=0, has_side_effects=True, vmem_limit_bytes=VMEM_LIMIT
        ),
        name="serve",
    )(*(pltpu.with_memory_space_constraint(a, pltpu.HBM) for a in operands))
    down, scale, router = pl.pallas_call(
        put_out,
        out_shape=outs,
        in_specs=[vmem] * 3,
        out_specs=(hbm,) * 3,
        scratch_shapes=[dma((12,))],
        compiler_params=pltpu.CompilerParams(vmem_limit_bytes=1024 * 1024),
        name="put_out",
    )(*served)
    return down, scale, router.T


def solution(mesh):
    return jax.shard_map(
        body,
        mesh=mesh,
        in_specs=(P("ep", None, "fsdp"), P("fsdp", "ep"), P("fsdp")),
        out_specs=(P("ep", "fsdp", None), P("ep", "fsdp"), P()),
        check_vma=False,
    )
```

```python
import jax
import jax.numpy as jnp
from jax import lax
from jax.experimental import pallas as pl
from jax.experimental.pallas import tpu as pltpu
from jax.sharding import PartitionSpec as P

MESH = pl.DeviceIdType.MESH
F32, BF16 = jnp.float32, jnp.bfloat16
Z, X, EP = 8, 4, 8
PARTNERS = Z * X
ROWS = 200
CHUNKS = 4
FIRST = 2
VMEM_LIMIT = 40_000_000
PRE = tuple((4, dx) for dx in range(X))
R = 24


NEAR = sorted(
    ((dz, dx) for dz in range(Z) for dx in range(X) if dz or dx),
    key=lambda o: (min(o[0], Z - o[0]) + min(o[1], X - o[1]), o),
)
ORDER = (
    [(dz, dx) for dx in range(X) for dz in (1, 7)]
    + [(0, dx) for dx in (1, 2, 3)]
    + [(4, dx) for dx in (2, 1, 3, 0)]
    + [(dz, dx) for dx in (2, 1, 3, 0) for dz in (3, 5, 2, 6)]
)


def row_sums(block):
    square = block * block
    total = jnp.broadcast_to(jnp.sum(square, axis=1, keepdims=True), square.shape)
    rows = lax.broadcasted_iota(jnp.int32, (128, 128), 0)
    own = rows == lax.broadcasted_iota(jnp.int32, (128, 128), 1)
    return jnp.concatenate(
        [
            jnp.sum(
                jnp.where(own[: min(128, 2 * ROWS - r)], total[r : r + 128], 0.0),
                axis=0,
                keepdims=True,
            )
            for r in range(0, 2 * ROWS, 128)
        ],
        axis=1,
    )


def serve(
    w_ref, weight_ref, gain_ref, down_ref, scale_ref, router_ref,
    w, weight, gain, part, landed, total, scales, early, send, product, rows, columns,
    load_sem, part_send, part_recv, scale_send, scale_recv,
    early_send, early_recv, down_send, down_recv, router_send, router_recv, product_send, product_recv,
):
    ep, me = lax.axis_index("ep"), lax.axis_index("fsdp")
    z, x = me // X, lax.rem(me, X)

    each = PARTNERS // CHUNKS
    loads = []
    for c in range(CHUNKS):
        piece = pl.ds(c * each * ROWS, each * ROWS)
        loads.append((w_ref.at[:, piece, :], w.at[:, piece, :]))
    loads += [(weight_ref, weight), (gain_ref, gain)]
    loads = [pltpu.make_async_copy(*pair, load_sem.at[i]) for i, pair in enumerate(loads)]
    for load in loads[:FIRST] + loads[CHUNKS:]:
        load.start(priority=0)
    for load in loads[FIRST:CHUNKS]:
        load.start(priority=1)

    barrier = pltpu.get_barrier_semaphore()
    zs = [lax.rem(z + d, Z) * X for d in range(Z)]
    xs = [lax.rem(x + d, X) for d in range(X)]
    partners = [zs[dz] + xs[dx] for dz, dx in NEAR]
    peers = [lax.rem(ep + d, EP) for d in range(1, EP)]
    for t in reversed(partners):
        pl.semaphore_signal(barrier, inc=1, device_id={"fsdp": t}, device_id_type=MESH)
    for e in peers:
        pl.semaphore_signal(barrier, inc=1, device_id={"ep": e}, device_id_type=MESH)

    loads[CHUNKS].wait()
    loads[CHUNKS + 1].wait()
    product[...] = (weight[...] * gain[...]).astype(BF16)

    def rows_of(t):
        block = w[:, pl.ds(pl.multiple_of(t * ROWS, 8), ROWS), :]
        return block.reshape(2 * ROWS, 128)

    for c in range(CHUNKS):
        loads[c].wait()

        @pl.loop(c * each, (c + 1) * each, unroll=each)
        def _(t):
            part[t] = row_sums(rows_of(t))

    pl.semaphore_wait(barrier, len(partners) + len(peers))
    for t in reversed(partners):
        pltpu.make_async_remote_copy(
            src_ref=part.at[t], dst_ref=landed.at[me], send_sem=part_send, recv_sem=part_recv,
            device_id={"fsdp": t}, device_id_type=MESH,
        ).start()

    for i, (dz, dx) in enumerate(PRE):
        t = zs[dz] + xs[dx]
        pltpu.make_async_remote_copy(
            src_ref=w.at[:, pl.ds(pl.multiple_of(t * ROWS, 8), R), :], dst_ref=early.at[i], send_sem=early_send, recv_sem=early_recv,
            device_id={"fsdp": t}, device_id_type=MESH,
        ).start()

    landed[me] = part[me]
    others = pl.ds(0, PARTNERS - 1)
    pltpu.make_async_copy(landed.at[others], landed.at[others], part_recv).wait()
    scale = jnp.sqrt(jnp.sum(landed[...], axis=0))
    total[...] = scale
    scales[me] = scale
    for e in range(2):
        scale_ref[e : e + 1] = scale[:, e * ROWS : (e + 1) * ROWS]
    for t in partners:
        pltpu.make_async_remote_copy(
            src_ref=total, dst_ref=scales.at[me], send_sem=scale_send, recv_sem=scale_recv.at[me],
            device_id={"fsdp": t}, device_id_type=MESH,
        ).start()

    lanes = pl.ds(pl.multiple_of(me * 128, 128), 128)
    rows[:, lanes] = product[...]
    for t in partners:
        pltpu.make_async_remote_copy(
            src_ref=product, dst_ref=rows.at[:, lanes], send_sem=product_send, recv_sem=product_recv,
            device_id={"fsdp": t}, device_id_type=MESH,
        ).start()

    def scaled(t):
        inverse = 1.0 / scales[t, :, 0 : 2 * ROWS]
        return (rows_of(t) * jnp.broadcast_to(inverse, (128, 2 * ROWS)).T).astype(BF16)

    def make(t, first):
        pltpu.make_async_copy(scales.at[t], scales.at[t], scale_recv.at[t]).wait()
        value = scaled(t)
        send[t, 0, first:] = value[first:ROWS]
        send[t, 1, first:] = value[ROWS + first:]

    def go(t, first):
        left, kind = pl.ds(first, ROWS - first), int(first > 0)
        pltpu.make_async_remote_copy(
            src_ref=send.at[t, :, left], dst_ref=down_ref.at[:, left, lanes], send_sem=down_send.at[kind], recv_sem=down_recv.at[kind],
            device_id={"fsdp": t}, device_id_type=MESH,
        ).start()

    last = None
    for o in ORDER:
        this = zs[o[0]] + xs[o[1]], R if o in PRE else 0
        make(*this)
        if last is not None:
            go(*last)
        last = this
    go(*last)

    some = rows.at[:, pl.ds(0, (PARTNERS - 1) * 128)]
    pltpu.make_async_copy(some, some, product_recv).wait()
    columns[ep] = rows[...]
    for e in peers:
        pltpu.make_async_remote_copy(
            src_ref=rows, dst_ref=columns.at[ep], send_sem=router_send, recv_sem=router_recv,
            device_id={"ep": e}, device_id_type=MESH,
        ).start()
    pltpu.make_async_copy(some, some, product_send).wait()

    few = early.at[pl.ds(0, len(PRE))]
    pltpu.make_async_copy(few, few, early_recv).wait()
    inverse = jnp.broadcast_to(1.0 / scale[:, 0:400], (128, 400)).T
    for i, (dz, dx) in enumerate(PRE):
        s = zs[(8 - dz) % 8] + xs[(4 - dx) % 4]
        for e in range(2):
            down_ref[e, 0:R, pl.ds(pl.multiple_of(s * 128, 128), 128)] = (early[i, e] * inverse[e * ROWS : e * ROWS + R]).astype(BF16)
    pltpu.make_async_copy(few, few, early_send).wait()

    own = scaled(me)
    down_ref[0, :, lanes] = own[:ROWS]
    down_ref[1, :, lanes] = own[ROWS:]

    pltpu.make_async_copy(columns.at[pl.ds(0, EP - 1)], columns.at[pl.ds(0, EP - 1)], router_recv).wait()
    for e in range(EP):
        router_ref[2 * e : 2 * e + 2, :] = columns[e]

    pltpu.make_async_copy(part.at[others], part.at[others], part_send).wait()
    pltpu.make_async_copy(scales.at[others], scales.at[others], scale_send).wait()
    pltpu.make_async_copy(columns.at[pl.ds(0, EP - 1)], columns.at[pl.ds(0, EP - 1)], router_send).wait()
    for sem in (down_send, down_recv):
        k = PARTNERS - 1 - len(PRE)
        pltpu.make_async_copy(send.at[pl.ds(0, k)], send.at[pl.ds(0, k)], sem.at[0]).wait()
        p = send.at[pl.ds(0, len(PRE)), :, pl.ds(R, ROWS - R)]
        pltpu.make_async_copy(p, p, sem.at[1]).wait()


def put_out(down_ref, scale_ref, router_ref, down_out, scale_out, router_out, sem):
    pairs = [(scale_ref, scale_out), (router_ref, router_out)]
    for e in range(2):
        pairs.append((down_ref.at[e], down_out.at[e]))
    copies = [pltpu.make_async_copy(*pair, sem.at[i]) for i, pair in enumerate(pairs)]
    for copy in copies:
        copy.start()
    for copy in copies:
        copy.wait()


def body(w_down, router_weight, router_gain):
    vmem, hbm = pl.BlockSpec(memory_space=pltpu.VMEM), pl.BlockSpec(memory_space=pltpu.HBM)
    dma = pltpu.SemaphoreType.DMA
    outs = (
        jax.ShapeDtypeStruct((2, ROWS, PARTNERS * 128), BF16),
        jax.ShapeDtypeStruct((2, ROWS), F32),
        jax.ShapeDtypeStruct((2 * EP, PARTNERS * 128), BF16),
    )
    operands = (w_down, router_weight.T, router_gain[None])
    served = pl.pallas_call(
        serve,
        out_shape=outs,
        in_specs=[hbm] * 3,
        out_specs=(vmem,) * 3,
        scratch_shapes=[
            pltpu.VMEM((2, PARTNERS * ROWS, 128), F32),
            pltpu.VMEM((2, 128), F32),
            pltpu.VMEM((1, 128), F32),
            pltpu.VMEM((PARTNERS, 1, 512), F32),
            pltpu.VMEM((PARTNERS, 1, 512), F32),
            pltpu.VMEM((1, 512), F32),
            pltpu.VMEM((PARTNERS, 1, 512), F32),
            pltpu.VMEM((len(PRE), 2, R, 128), F32),
            pltpu.VMEM((PARTNERS, 2, ROWS, 128), BF16),
            pltpu.VMEM((2, 128), BF16),
            pltpu.VMEM((2, PARTNERS * 128), BF16),
            pltpu.VMEM((EP, 2, PARTNERS * 128), BF16),
            dma((CHUNKS + 2,)), dma, dma, dma, dma((PARTNERS,)), dma, dma, dma((2,)), dma((2,)), dma, dma, dma, dma,
        ],
        compiler_params=pltpu.CompilerParams(
            collective_id=0, has_side_effects=True, vmem_limit_bytes=VMEM_LIMIT
        ),
        name="serve",
    )(*(pltpu.with_memory_space_constraint(a, pltpu.HBM) for a in operands))
    down, scale, router = pl.pallas_call(
        put_out,
        out_shape=outs,
        in_specs=[vmem] * 3,
        out_specs=(hbm,) * 3,
        scratch_shapes=[dma((4,))],
        compiler_params=pltpu.CompilerParams(vmem_limit_bytes=1024 * 1024),
        name="put_out",
    )(*served)
    return down, scale, router.T


def solution(mesh):
    return jax.shard_map(
        body,
        mesh=mesh,
        in_specs=(P("ep", None, "fsdp"), P("fsdp", "ep"), P("fsdp")),
        out_specs=(P("ep", "fsdp", None), P("ep", "fsdp"), P()),
        check_vma=False,
    )
```

```python
import jax
import jax.numpy as jnp
from jax import lax
from jax.experimental import pallas as pl
from jax.experimental.pallas import tpu as pltpu
from jax.sharding import PartitionSpec as P

MESH = pl.DeviceIdType.MESH
F32, BF16 = jnp.float32, jnp.bfloat16
Z, X, EP = 8, 4, 8
PARTNERS = Z * X
ROWS = 200
CHUNKS = 4
FIRST = 2
VMEM_LIMIT = 40_000_000
PRE = tuple((4, dx) for dx in range(X))
R = 24


NEAR = sorted(
    ((dz, dx) for dz in range(Z) for dx in range(X) if dz or dx),
    key=lambda o: (min(o[0], Z - o[0]) + min(o[1], X - o[1]), o),
)
ORDER = (
    [(dz, dx) for dx in range(X) for dz in (1, 7)]
    + [(0, dx) for dx in (1, 2, 3)]
    + [(4, dx) for dx in (2, 1, 3, 0)]
    + [(dz, dx) for dx in (2, 1, 3, 0) for dz in (3, 5, 2, 6)]
)


def row_sums(block):
    square = block * block
    total = jnp.broadcast_to(jnp.sum(square, axis=1, keepdims=True), square.shape)
    rows = lax.broadcasted_iota(jnp.int32, (128, 128), 0)
    own = rows == lax.broadcasted_iota(jnp.int32, (128, 128), 1)
    return jnp.concatenate(
        [
            jnp.sum(
                jnp.where(own[: min(128, 2 * ROWS - r)], total[r : r + 128], 0.0),
                axis=0,
                keepdims=True,
            )
            for r in range(0, 2 * ROWS, 128)
        ],
        axis=1,
    )


def serve(
    w_ref, weight_ref, gain_ref, down_ref, scale_ref, router_ref,
    w, weight, gain, part, landed, total, scales, early, send, product, rows, columns,
    load_sem, part_send, part_recv, scale_send, scale_recv,
    early_send, early_recv, down_send, down_recv, router_send, router_recv, product_send, product_recv,
):
    ep, me = lax.axis_index("ep"), lax.axis_index("fsdp")
    z, x = me // X, lax.rem(me, X)

    each = PARTNERS // CHUNKS
    loads = []
    for c in range(CHUNKS):
        piece = pl.ds(c * each * ROWS, each * ROWS)
        loads.append((w_ref.at[:, piece, :], w.at[:, piece, :]))
    loads += [(weight_ref, weight), (gain_ref, gain)]
    loads = [pltpu.make_async_copy(*pair, load_sem.at[i]) for i, pair in enumerate(loads)]
    for load in loads[:FIRST]:
        load.start(priority=0)

    barrier = pltpu.get_barrier_semaphore()
    zs = [lax.rem(z + d, Z) * X for d in range(Z)]
    xs = [lax.rem(x + d, X) for d in range(X)]
    partners = [zs[dz] + xs[dx] for dz, dx in NEAR]
    peers = [lax.rem(ep + d, EP) for d in range(1, EP)]
    for t in reversed(partners):
        pl.semaphore_signal(barrier, inc=1, device_id={"fsdp": t}, device_id_type=MESH)
    for e in peers:
        pl.semaphore_signal(barrier, inc=1, device_id={"ep": e}, device_id_type=MESH)

    for load in loads[FIRST:CHUNKS]:
        load.start(priority=1)
    for load in loads[CHUNKS:]:
        load.start()


    def rows_of(t):
        block = w[:, pl.ds(pl.multiple_of(t * ROWS, 8), ROWS), :]
        return block.reshape(2 * ROWS, 128)

    for c in range(CHUNKS):
        loads[c].wait()

        @pl.loop(c * each, (c + 1) * each, unroll=each)
        def _(t):
            part[t] = row_sums(rows_of(t))

    pl.semaphore_wait(barrier, len(partners) + len(peers))
    for t in reversed(partners):
        pltpu.make_async_remote_copy(
            src_ref=part.at[t], dst_ref=landed.at[me], send_sem=part_send, recv_sem=part_recv,
            device_id={"fsdp": t}, device_id_type=MESH,
        ).start()

    for i, (dz, dx) in enumerate(PRE):
        t = zs[dz] + xs[dx]
        pltpu.make_async_remote_copy(
            src_ref=w.at[:, pl.ds(pl.multiple_of(t * ROWS, 8), R), :], dst_ref=early.at[i], send_sem=early_send, recv_sem=early_recv,
            device_id={"fsdp": t}, device_id_type=MESH,
        ).start()

    landed[me] = part[me]
    loads[CHUNKS].wait()
    loads[CHUNKS + 1].wait()
    product[...] = (weight[...] * gain[...]).astype(BF16)
    others = pl.ds(0, PARTNERS - 1)
    pltpu.make_async_copy(landed.at[others], landed.at[others], part_recv).wait()
    scale = jnp.sqrt(jnp.sum(landed[...], axis=0))
    total[...] = scale
    scales[me] = scale
    for e in range(2):
        scale_ref[e : e + 1] = scale[:, e * ROWS : (e + 1) * ROWS]
    for t in partners:
        pltpu.make_async_remote_copy(
            src_ref=total, dst_ref=scales.at[me], send_sem=scale_send, recv_sem=scale_recv.at[me],
            device_id={"fsdp": t}, device_id_type=MESH,
        ).start()

    lanes = pl.ds(pl.multiple_of(me * 128, 128), 128)
    rows[:, lanes] = product[...]
    for t in partners:
        pltpu.make_async_remote_copy(
            src_ref=product, dst_ref=rows.at[:, lanes], send_sem=product_send, recv_sem=product_recv,
            device_id={"fsdp": t}, device_id_type=MESH,
        ).start()

    def scaled(t):
        inverse = 1.0 / scales[t, :, 0 : 2 * ROWS]
        return (rows_of(t) * jnp.broadcast_to(inverse, (128, 2 * ROWS)).T).astype(BF16)

    def make(t, first):
        pltpu.make_async_copy(scales.at[t], scales.at[t], scale_recv.at[t]).wait()
        value = scaled(t)
        send[t, 0, first:] = value[first:ROWS]
        send[t, 1, first:] = value[ROWS + first:]

    def go(t, first):
        left, kind = pl.ds(first, ROWS - first), int(first > 0)
        pltpu.make_async_remote_copy(
            src_ref=send.at[t, :, left], dst_ref=down_ref.at[:, left, lanes], send_sem=down_send.at[kind], recv_sem=down_recv.at[kind],
            device_id={"fsdp": t}, device_id_type=MESH,
        ).start()

    last = None
    for o in ORDER:
        this = zs[o[0]] + xs[o[1]], R if o in PRE else 0
        make(*this)
        if last is not None:
            go(*last)
        last = this
    go(*last)

    some = rows.at[:, pl.ds(0, (PARTNERS - 1) * 128)]
    pltpu.make_async_copy(some, some, product_recv).wait()
    columns[ep] = rows[...]
    for e in peers:
        pltpu.make_async_remote_copy(
            src_ref=rows, dst_ref=columns.at[ep], send_sem=router_send, recv_sem=router_recv,
            device_id={"ep": e}, device_id_type=MESH,
        ).start()
    pltpu.make_async_copy(some, some, product_send).wait()

    few = early.at[pl.ds(0, len(PRE))]
    pltpu.make_async_copy(few, few, early_recv).wait()
    inverse = jnp.broadcast_to(1.0 / scale[:, 0:400], (128, 400)).T
    for i, (dz, dx) in enumerate(PRE):
        s = zs[(8 - dz) % 8] + xs[(4 - dx) % 4]
        for e in range(2):
            down_ref[e, 0:R, pl.ds(pl.multiple_of(s * 128, 128), 128)] = (early[i, e] * inverse[e * ROWS : e * ROWS + R]).astype(BF16)
    pltpu.make_async_copy(few, few, early_send).wait()

    own = scaled(me)
    down_ref[0, :, lanes] = own[:ROWS]
    down_ref[1, :, lanes] = own[ROWS:]

    pltpu.make_async_copy(columns.at[pl.ds(0, EP - 1)], columns.at[pl.ds(0, EP - 1)], router_recv).wait()
    for e in range(EP):
        router_ref[2 * e : 2 * e + 2, :] = columns[e]

    pltpu.make_async_copy(part.at[others], part.at[others], part_send).wait()
    pltpu.make_async_copy(scales.at[others], scales.at[others], scale_send).wait()
    pltpu.make_async_copy(columns.at[pl.ds(0, EP - 1)], columns.at[pl.ds(0, EP - 1)], router_send).wait()
    for sem in (down_send, down_recv):
        k = PARTNERS - 1 - len(PRE)
        pltpu.make_async_copy(send.at[pl.ds(0, k)], send.at[pl.ds(0, k)], sem.at[0]).wait()
        p = send.at[pl.ds(0, len(PRE)), :, pl.ds(R, ROWS - R)]
        pltpu.make_async_copy(p, p, sem.at[1]).wait()


def put_out(down_ref, scale_ref, router_ref, down_out, scale_out, router_out, sem):
    pairs = [(scale_ref, scale_out), (router_ref, router_out)]
    for e in range(2):
        pairs.append((down_ref.at[e], down_out.at[e]))
    copies = [pltpu.make_async_copy(*pair, sem.at[i]) for i, pair in enumerate(pairs)]
    for copy in reversed(copies):
        copy.start()
    for copy in copies:
        copy.wait()


def body(w_down, router_weight, router_gain):
    vmem, hbm = pl.BlockSpec(memory_space=pltpu.VMEM), pl.BlockSpec(memory_space=pltpu.HBM)
    dma = pltpu.SemaphoreType.DMA
    outs = (
        jax.ShapeDtypeStruct((2, ROWS, PARTNERS * 128), BF16),
        jax.ShapeDtypeStruct((2, ROWS), F32),
        jax.ShapeDtypeStruct((2 * EP, PARTNERS * 128), BF16),
    )
    operands = (w_down, router_weight.T, router_gain[None])
    served = pl.pallas_call(
        serve,
        out_shape=outs,
        in_specs=[hbm] * 3,
        out_specs=(vmem,) * 3,
        scratch_shapes=[
            pltpu.VMEM((2, PARTNERS * ROWS, 128), F32),
            pltpu.VMEM((2, 128), F32),
            pltpu.VMEM((1, 128), F32),
            pltpu.VMEM((PARTNERS, 1, 512), F32),
            pltpu.VMEM((PARTNERS, 1, 512), F32),
            pltpu.VMEM((1, 512), F32),
            pltpu.VMEM((PARTNERS, 1, 512), F32),
            pltpu.VMEM((len(PRE), 2, R, 128), F32),
            pltpu.VMEM((PARTNERS, 2, ROWS, 128), BF16),
            pltpu.VMEM((2, 128), BF16),
            pltpu.VMEM((2, PARTNERS * 128), BF16),
            pltpu.VMEM((EP, 2, PARTNERS * 128), BF16),
            dma((CHUNKS + 2,)), dma, dma, dma, dma((PARTNERS,)), dma, dma, dma((2,)), dma((2,)), dma, dma, dma, dma,
        ],
        compiler_params=pltpu.CompilerParams(
            collective_id=0, has_side_effects=True, vmem_limit_bytes=VMEM_LIMIT
        ),
        name="serve",
    )(*(pltpu.with_memory_space_constraint(a, pltpu.HBM) for a in operands))
    down, scale, router = pl.pallas_call(
        put_out,
        out_shape=outs,
        in_specs=[vmem] * 3,
        out_specs=(hbm,) * 3,
        scratch_shapes=[dma((4,))],
        compiler_params=pltpu.CompilerParams(vmem_limit_bytes=1024 * 1024),
        name="put_out",
    )(*served)
    return down, scale, router.T


def solution(mesh):
    return jax.shard_map(
        body,
        mesh=mesh,
        in_specs=(P("ep", None, "fsdp"), P("fsdp", "ep"), P("fsdp")),
        out_specs=(P("ep", "fsdp", None), P("ep", "fsdp"), P()),
        check_vma=False,
    )
```
